512 devices in a mesh: tile: 64 (over z, x, core), mem: 8 (over y).
Axes of the slice: x: 4, y: 8, z: 8, core: 2. Of those that a mesh axis runs over, the one named last changes fastest.
Arguments:
- anomalies: bfloat16 [80, 137, 8192], P('mem', None, 'tile'), may hold values from -6 to 6
- analysis_weights: bfloat16 [64, 80, 80], P('tile'), may hold values from -0.6 to 1.7
- background_mean: bfloat16 [137, 8192], P(None, 'tile'), may hold values from -6 to 6
- background: bfloat16 [80, 137, 8192], P('mem', None, 'tile'), may hold values from -6 to 6
- jacobian_table: bfloat16 [8461, 137], replicated, may hold values from -0.5 to 0.5
- channel_list: int32 [96], replicated, may hold values from 0 to 8460
- send_slots: int32 [64, 64, 32], P('tile'), may hold values from -1 to 127, as said below
- footprint: int32 [32768, 4], P('tile'), may hold values from 0 to 2047, as said below
- footprint_weight: bfloat16 [32768, 4], P('tile'), may hold values from 0.25 to 1
- channel_bias: float32 [96], replicated, may hold values from -4 to 4
Outputs:
- analysis_members: bfloat16 [80, 137, 8192], P('mem', None, 'tile')
- radiance_prior: float32 [96, 80, 32768], P(None, 'mem', 'tile')
The draws below stay inside these ranges and needn't reach their ends.
Inputs may be any that keep to these rules, and one draw needn't show every extreme that they name: `send_slots`: entry [s, d, i] is a column within owner s's block of 128 columns that owner s sends to tile d in slot i, or -1 for an empty slot; the filled slots of a pair come first, each pair fills 1 to 32 slots, and in every draw one tile receives 32 filled slots from every owner. `footprint`: entry [o, j] is a slot of the buffer of observation o's tile, which holds 32 slots from each owner in owner order; every entry names a filled slot, the 4 entries of a row differ, and every filled slot is named by some row of that tile.
All inputs are finite; a program needn't handle non-finite values.
Results may differ from the reference program's by a relative error of at most 0.0021.
Values may be sent and summed in bfloat16 or wider, within the bound.
No kernel may reach another device: no remote copies, remote signals or barrier semaphores. Data moves between devices by JAX's collectives and lax.ppermute only.
A program may use at most 128 MiB of HBM per device.

```python
import math
import jax
import jax.numpy as jnp
from jax import lax

MEMBERS = 80
LEVELS = 137
SPECTRUM = 8461
CHANNELS = 96
COLS_DEV = 128
GROUP = 128
SLOTS = 32
OBS_DEV = 512
FOOT = 4
COLUMNS = 8192
POINTS = 64
OBSERVATIONS = 32768
N_TILE = 64


def draw_analysis_weights(key, part):
    identity = jnp.eye(MEMBERS, dtype=jnp.float32)[None]
    noise_draw = jnp.clip(jax.random.normal(jax.random.fold_in(key, 1), (POINTS, MEMBERS, MEMBERS), jnp.float32), -4.0, 4.0)
    diag_part = identity
    return (diag_part + noise_draw * (0.6 / math.sqrt(MEMBERS))).astype(jnp.bfloat16)


def slot_counts(key):
    tile_count = COLUMNS // COLS_DEV
    uniform_part = jax.random.randint(jax.random.fold_in(key, 11), (tile_count, tile_count), 1, SLOTS + 1)
    receiver_load = jax.random.randint(jax.random.fold_in(key, 12), (1, tile_count), 1, 5)
    counts = jnp.clip(uniform_part * receiver_load // 3, 1, SLOTS)
    full_receiver = jax.random.randint(jax.random.fold_in(key, 13), (), 0, tile_count)
    counts = jnp.where(jnp.arange(tile_count)[None, :] == full_receiver, SLOTS, counts)
    return counts.astype(jnp.int32)


def draw_send_slots(key, part):
    tile_count = COLUMNS // COLS_DEV
    counts = slot_counts(key)
    columns = jax.random.randint(jax.random.fold_in(key, 14), (tile_count, tile_count, SLOTS), 0, COLS_DEV)
    filled = jnp.arange(SLOTS)[None, None, :] < counts[:, :, None]
    return jnp.where(filled, columns, -1).astype(jnp.int32)


def draw_footprint(key, part):
    tile_count = COLUMNS // COLS_DEV
    buffer_size = tile_count * SLOTS
    counts = slot_counts(key)
    filled = jnp.arange(SLOTS)[None, None, :] < jnp.transpose(counts)[:, :, None]
    filled = filled.reshape(tile_count, buffer_size)
    receiver_keys = jax.random.split(jax.random.fold_in(key, 15), tile_count)

    def shuffle_one(subkey):
        return jax.random.permutation(subkey, buffer_size).astype(jnp.int32)
    shuffle = jax.vmap(shuffle_one)(receiver_keys)
    scores = jnp.where(filled, shuffle, buffer_size + shuffle)
    slot_order = jnp.argsort(scores, axis=1, stable=True).astype(jnp.int32)
    filled_count = jnp.sum(filled.astype(jnp.int32), axis=1, keepdims=True)
    position = jnp.arange(OBS_DEV * FOOT, dtype=jnp.int32)[None, :] % filled_count
    foot_slots = jnp.take_along_axis(slot_order, position, axis=1)
    return foot_slots.reshape(tile_count * OBS_DEV, FOOT).astype(jnp.int32)


def set_ends(entries, stream_key, low, high):
    longest = entries.shape.index(max(entries.shape))
    spots = []
    for shift in (0, 1):
        where = [jax.random.randint(jax.random.fold_in(stream_key, axis), (), 0, length) for axis, length in enumerate(entries.shape)]
        where[longest] = (where[longest] + shift) % entries.shape[longest]
        spots.append(tuple(where))
    return entries.at[spots[0]].set(low).at[spots[1]].set(high)


def levels(key, extent, shards, low, largest):
    factor_of = 1.0
    for dim, parts in shards:
        draws = jax.random.uniform(jax.random.fold_in(jax.random.fold_in(key, 6), dim), (parts,), jnp.float32, low / len(shards), largest / len(shards))
        factor_of = factor_of * jnp.repeat(jnp.exp(draws), extent[dim] // parts).reshape((-1,) + (1,) * (len(extent) - 1 - dim))
    return factor_of


def gaussian(rng, shape, scale, limit, shards=(), kind=jnp.bfloat16):
    values = scale * jax.random.normal(rng, shape, jnp.float32)
    if shards:
        values = values * levels(rng, shape, shards, -0.22, 0.18)
    return jnp.clip(values, -limit, limit).astype(kind)


def setup_inputs(seed: int = 0) -> dict:
    key_list = jax.random.split(jax.random.key(seed), 11)
    anomalies = gaussian(key_list[0], (MEMBERS, LEVELS, COLUMNS), 1.0, 6.0, ((0, 8), (2, 64)))
    analysis_weights = draw_analysis_weights(jax.random.fold_in(key_list[10], 71), 0)
    background_mean = gaussian(key_list[2], (LEVELS, COLUMNS), 1.0, 6.0, ((1, 64),))
    background = gaussian(key_list[3], (MEMBERS, LEVELS, COLUMNS), 1.0, 6.0, ((0, 8), (2, 64)))
    jacobian_table = gaussian(key_list[4], (SPECTRUM, LEVELS), LEVELS ** -0.5, 0.5)
    channel_list = set_ends(jax.random.randint(key_list[5], (CHANNELS,), 0, SPECTRUM), jax.random.fold_in(key_list[5], 1), 0, SPECTRUM - 1).astype(jnp.int32)
    send_slots = draw_send_slots(jax.random.fold_in(key_list[10], 71), 0)
    footprint = draw_footprint(jax.random.fold_in(key_list[10], 71), 0)
    footprint_weight = jnp.clip(jnp.exp(math.log(1.0) - 1.3862944 * jax.random.uniform(key_list[8], (OBSERVATIONS, FOOT), jnp.float32) ** levels(key_list[8], (OBSERVATIONS, FOOT), ((0, 64),), -0.2, 0.2)), 0.25, 1.0).astype(jnp.bfloat16)
    channel_bias = gaussian(key_list[9], (CHANNELS,), 1.0, 4.0, (), jnp.float32)
    return {"anomalies": anomalies, "analysis_weights": analysis_weights, "background_mean": background_mean, "background": background, "jacobian_table": jacobian_table, "channel_list": channel_list, "send_slots": send_slots, "footprint": footprint, "footprint_weight": footprint_weight, "channel_bias": channel_bias}


def reference(anomalies, analysis_weights, background_mean, background, jacobian_table, channel_list, send_slots, footprint, footprint_weight, channel_bias):
    points = analysis_weights.shape[0]
    shaped = anomalies.astype(jnp.float32).reshape(MEMBERS, LEVELS, points, GROUP)
    mixture = jnp.einsum('klgc,gkm->mlgc', shaped, analysis_weights.astype(jnp.float32))
    mixture = mixture.reshape(MEMBERS, LEVELS, points * GROUP)
    analysis_members = (background_mean.astype(jnp.float32)[None] + mixture).astype(jnp.bfloat16)

    selected = jnp.take(jacobian_table, channel_list, axis=0).astype(jnp.float32)
    foot_slots = footprint.reshape(N_TILE, OBS_DEV, FOOT)
    foot_weight = footprint_weight.astype(jnp.float32).reshape(N_TILE, OBS_DEV, FOOT)

    def per_receiver(receiver):
        slot_ids = lax.dynamic_index_in_dim(foot_slots, receiver, 0, keepdims=False)
        weight = lax.dynamic_index_in_dim(foot_weight, receiver, 0, keepdims=False)
        source = (slot_ids // SLOTS).astype(jnp.int32)
        slot_place = (slot_ids % SLOTS).astype(jnp.int32)
        local_col = send_slots[source, receiver, slot_place]
        column = (source * COLS_DEV + local_col).astype(jnp.int32)
        profiles = jnp.take(background, column.reshape(-1), axis=2).astype(jnp.float32)
        radiance = jnp.einsum('cl,kls->cks', selected, profiles).astype(jnp.bfloat16)
        radiance = lax.optimization_barrier(radiance).astype(jnp.float32)
        radiance = radiance.reshape(CHANNELS, MEMBERS, OBS_DEV, FOOT)
        combined = jnp.sum(radiance * weight[None, None], axis=3)
        return combined + channel_bias.astype(jnp.float32)[:, None, None]

    stacked = lax.map(per_receiver, jnp.arange(N_TILE, dtype=jnp.int32))
    radiance_prior = jnp.transpose(stacked, (1, 2, 0, 3)).reshape(CHANNELS, MEMBERS, N_TILE * OBS_DEV)
    return analysis_members, radiance_prior
```

```python
import jax
import jax.numpy as jnp
from jax import lax
from jax.sharding import PartitionSpec as P

SLOTS = 32
FOOT = 4
f32 = jnp.float32
bf16 = jnp.bfloat16


def shards(
    anomalies,
    analysis_weights,
    background_mean,
    background,
    jacobian_table,
    channel_list,
    send_slots,
    footprint,
    footprint_weight,
    channel_bias,
):
    mem_dev, levels, cols = anomalies.shape
    spectrum = jacobian_table.shape[0]
    channels = channel_list.shape[0]
    tiles = send_slots.shape[1]
    obs = footprint.shape[0]
    n_mem = lax.axis_size("mem")
    members = n_mem * mem_dev
    feats = mem_dev * channels

    pick = (channel_list[:, None] == lax.broadcasted_iota(jnp.int32, (channels, spectrum), 1)).astype(bf16)
    selected = jnp.einsum("cv,vl->cl", pick, jacobian_table, preferred_element_type=f32).astype(bf16)
    owned = jnp.einsum("klx,cl->xkc", background, selected, preferred_element_type=f32).astype(bf16)
    owned = owned.reshape(cols, feats)
    slots = jnp.maximum(send_slots[0], 0)
    slot_pick = (slots[:, :, None] == lax.broadcasted_iota(jnp.int32, (tiles, SLOTS, cols), 2)).astype(bf16)
    packed = jnp.einsum("dsx,xf->dsf", slot_pick, owned, preferred_element_type=f32).astype(bf16)
    received = lax.all_to_all(packed, "tile", 0, 0)

    block = -(-levels // n_mem)
    padded = jnp.pad(anomalies, ((0, 0), (0, block * n_mem - levels), (0, 0)))
    pieces = padded.reshape(mem_dev, n_mem, block, cols).transpose(1, 0, 2, 3).reshape(n_mem, mem_dev * block, cols)
    pieces = lax.all_to_all(pieces, "mem", 0, 0).reshape(members, block, cols)
    mixed = jnp.einsum("klc,km->mlc", pieces, analysis_weights[0], preferred_element_type=f32)
    mean = jnp.pad(background_mean, ((0, block * n_mem - levels), (0, 0)))
    mean = lax.dynamic_slice_in_dim(mean, lax.axis_index("mem") * block, block, 0)
    done = (mixed + mean.astype(f32)[None]).astype(bf16).reshape(n_mem, mem_dev * block, cols)
    done = lax.all_to_all(done, "mem", 0, 0).reshape(n_mem, mem_dev, block, cols)
    analysis_members = done.transpose(1, 0, 2, 3).reshape(mem_dev, n_mem * block, cols)[:, :levels]

    rows = lax.broadcasted_iota(jnp.int32, (tiles * SLOTS, obs), 0)
    weight = jnp.zeros((tiles * SLOTS, obs), f32)
    for j in range(FOOT):
        weight = jnp.where(rows == footprint[:, j][None], footprint_weight[:, j].astype(f32)[None], weight)
    prior = jnp.einsum(
        "sf,so->fo", received.reshape(tiles * SLOTS, feats), weight.astype(bf16), preferred_element_type=f32
    )
    prior = prior.reshape(mem_dev, channels, obs) + channel_bias[None, :, None]
    return (analysis_members, prior.transpose(1, 0, 2))


def solution(mesh):
    placed = (
        P("mem", None, "tile"),
        P("tile", None, None),
        P(None, "tile"),
        P("mem", None, "tile"),
        P(),
        P(),
        P("tile", None, None),
        P("tile", None),
        P("tile", None),
        P(),
    )
    return jax.shard_map(
        shards,
        mesh=mesh,
        in_specs=placed,
        out_specs=(P("mem", None, "tile"), P(None, "mem", "tile")),
        check_vma=False,
    )
```

```python
import functools

import jax
import jax.numpy as jnp
from jax import lax
from jax.experimental import pallas as pl
from jax.experimental.layout import Layout, with_layout_constraint
from jax.experimental.pallas import tpu as pltpu
from jax.sharding import Mesh
from jax.sharding import PartitionSpec as P

SLOTS = 32
FOOT = 4
NZ, NX, NC = 8, 4, 2
f32 = jnp.float32
bf16 = jnp.bfloat16
TILE = ("z", "x", "c")
PARTS = ((0, 1, 7, 2), (6, 3, 5, 4))
GROUPS = 4


def vmem(n):
    return [pl.BlockSpec(memory_space=pltpu.VMEM)] * n


def params():
    return pltpu.CompilerParams(vmem_limit_bytes=24 * 2**20)


def radiance_kernel(sel_ref, back_ref, slots_ref, out_ref):
    members, channels = back_ref.shape[0], sel_ref.shape[0]
    sel = sel_ref[...]
    for k in range(members):
        got = jnp.dot(sel, back_ref[k], preferred_element_type=f32)
        out_ref[k * channels : (k + 1) * channels, :] = got.astype(bf16)
    out_ref[members * channels :, :] = slots_ref[...]


def radiance(sel, back, slots):
    rows = back.shape[0] * sel.shape[0] + slots.shape[0]
    return pl.pallas_call(
        radiance_kernel,
        out_shape=jax.ShapeDtypeStruct((rows, back.shape[2]), bf16),
        in_specs=vmem(3),
        out_specs=vmem(1)[0],
        compiler_params=params(),
        cost_estimate=pl.CostEstimate(flops=2_000_000_000, bytes_accessed=800_000, transcendentals=0),
        name="radiance",
    )(sel, back, slots)


def pack_kernel(feats, me_ref, *refs):
    blocks, out_ref = refs[:-1], refs[-1]
    cols = blocks[0].shape[1]
    peers = out_ref.shape[0]
    tail = blocks[0].shape[0] - feats
    group = lax.broadcasted_iota(jnp.int32, (8, cols), 1) // SLOTS
    row = lax.broadcasted_iota(jnp.int32, (tail, cols), 0)
    halves = peers // GROUPS
    rolled = []
    for b, block in enumerate(blocks):
        lists = block[feats:, :].astype(f32)
        for h in range(halves):
            mine = jnp.sum(jnp.where(row == me_ref[0] * halves + h, lists, 0.0), axis=0, keepdims=True)
            mine = jnp.broadcast_to(mine, (8, cols))
            rolled.append(pltpu.roll(mine, SLOTS * b, 1) if b else mine)
    col = lax.broadcasted_iota(jnp.int32, (cols, cols), 0).astype(f32)
    lane_group = lax.broadcasted_iota(jnp.int32, (cols, cols), 1) // SLOTS
    left = jnp.concatenate([block[:feats, :] for block in blocks], axis=1)
    for j0 in range(0, peers, 2):
        right = []
        for j in (j0, j0 + 1):
            want = jnp.full((8, cols), -1.0, f32)
            for b in range(GROUPS):
                want = jnp.where(group == (j + b) % GROUPS, rolled[b * halves + j // GROUPS], want)
            want = want[0:1, :]
            same = jnp.broadcast_to(want, (cols, cols)) == col
            right.append(
                jnp.concatenate(
                    [
                        jnp.where(same & (lane_group == (j + b) % GROUPS), 1.0, 0.0).astype(bf16)
                        for b in range(GROUPS)
                    ],
                    axis=0,
                )
            )
        got = jnp.dot(left, jnp.concatenate(right, axis=1), preferred_element_type=f32).astype(bf16)
        out_ref[j0] = got[:, :cols]
        out_ref[j0 + 1] = got[:, cols:]


def pack(blocks, me, feats):
    peers, cols = NX * NC, blocks[0].shape[1]
    return pl.pallas_call(
        functools.partial(pack_kernel, feats),
        out_shape=jax.ShapeDtypeStruct((peers, feats, cols), bf16),
        in_specs=[pl.BlockSpec(memory_space=pltpu.SMEM)] + vmem(len(blocks)),
        out_specs=vmem(1)[0],
        compiler_params=params(),
        cost_estimate=pl.CostEstimate(flops=2_500_000_000, bytes_accessed=3_000_000, transcendentals=0),
        name="pack",
    )(me, *blocks)


def spread_kernel(row_ref, weight_ref, out_ref):
    rows, obs = out_ref.shape
    step = 128

    @pl.loop(0, rows // step)
    def _(i):
        base = i * step
        row = lax.broadcasted_iota(jnp.int32, (step, obs), 0) + base
        total = jnp.zeros((step, obs), f32)
        for j in range(FOOT):
            total = jnp.where(row == row_ref[j : j + 1, :], weight_ref[j : j + 1, :], total)
        out_ref[pl.ds(pl.multiple_of(base, step), step), :] = total.astype(bf16)


def spread(row, weight, rows):
    return pl.pallas_call(
        spread_kernel,
        out_shape=jax.ShapeDtypeStruct((rows, row.shape[1]), bf16),
        in_specs=vmem(2),
        out_specs=vmem(1)[0],
        compiler_params=params(),
        cost_estimate=pl.CostEstimate(flops=rows * 1_500_000, bytes_accessed=rows * 1024, transcendentals=0),
        name="spread",
    )(row, weight)


def combine_kernel(got_ref, weight_ref, base_ref, out_ref):
    left = jnp.concatenate([got_ref[j] for j in range(got_ref.shape[0])], axis=1)
    out_ref[...] = jnp.dot(left, weight_ref[...], preferred_element_type=f32) + base_ref[...]


def combine(got, weight, base):
    peers, feats, width = got.shape
    obs = weight.shape[1]
    step = feats // 4
    return pl.pallas_call(
        combine_kernel,
        grid=(feats // step,),
        out_shape=jax.ShapeDtypeStruct((feats, obs), f32),
        in_specs=[
            pl.BlockSpec((peers, step, width), lambda i: (0, i, 0)),
            pl.BlockSpec(weight.shape, lambda i: (0, 0)),
            pl.BlockSpec((step, base.shape[1]), lambda i: (i, 0)),
        ],
        out_specs=pl.BlockSpec((step, obs), lambda i: (i, 0)),
        compiler_params=params(),
        cost_estimate=pl.CostEstimate(flops=4_000_000_000, bytes_accessed=5_000_000, transcendentals=0),
        name="combine",
    )(got, weight, base)


def shift(block, axis, size, ahead):
    return lax.ppermute(block, axis, [((i + ahead) % size, i) for i in range(size)])


def ring(block, axis, size):
    back = [(i, (i - 1) % size) for i in range(size)]
    ahead = [(i, (i + 1) % size) for i in range(size)]
    blocks = {0: block}
    for r in range(1, size // 2 + 1):
        blocks[r] = lax.ppermute(blocks[r - 1], axis, back)
        if r < size - r:
            blocks[size - r] = lax.ppermute(blocks[(size - r + 1) % size], axis, ahead)
    return blocks


def shards(
    anomalies,
    analysis_weights,
    background_mean,
    background,
    jacobian_table,
    channel_list,
    send_slots,
    footprint,
    footprint_weight,
    channel_bias,
):
    mem_dev, levels, cols = anomalies.shape
    spectrum = jacobian_table.shape[0]
    channels = channel_list.shape[0]
    tiles = send_slots.shape[1]
    obs = footprint.shape[0]
    n_mem = lax.axis_size("mem")
    feats = mem_dev * channels
    peers = NX * NC
    me_z = lax.axis_index("z")
    me_mem = lax.axis_index("mem")

    pick = (channel_list[:, None] == lax.broadcasted_iota(jnp.int32, (channels, spectrum), 1)).astype(bf16)
    selected = jnp.einsum("cv,vl->cl", pick, jacobian_table, preferred_element_type=f32).astype(bf16)
    slots = send_slots[0].reshape(tiles * SLOTS // cols, cols).astype(bf16)
    owned = radiance(selected, background, slots)

    blocks = {0: owned}
    for ahead in (1, 7, 2, 6):
        blocks[ahead] = shift(owned, "z", NZ, ahead)
    blocks[3] = shift(blocks[2], "z", NZ, 1)
    blocks[5] = shift(blocks[6], "z", NZ, 7)
    blocks[4] = shift(blocks[2], "z", NZ, 2)

    slot = footprint.T
    ahead = (slot // (peers * SLOTS) - me_z) % NZ
    peer, place = (slot // SLOTS) % peers, slot % SLOTS
    weight = footprint_weight.T.astype(f32)
    mine = lax.axis_index("x") * NC + lax.axis_index("c")
    prior = jnp.broadcast_to(channel_bias[None, :, None], (mem_dev, channels, 1)).reshape(feats, 1)
    for part in PARTS:
        sent = pack([blocks[r] for r in part], me_z.reshape(1), feats)
        got = lax.all_to_all(sent, ("x", "c"), 0, 0)
        row = jnp.full((FOOT, obs), -1, jnp.int32)
        for b, r in enumerate(part):
            row = jnp.where(ahead == r, (peer * GROUPS + (mine + b) % GROUPS) * SLOTS + place, row)
        prior = combine(got, spread(row, weight, peers * GROUPS * SLOTS), prior)

    pieces = ring(anomalies, "mem", n_mem)
    pieces = jnp.concatenate([pieces[r] for r in range(n_mem)], axis=0)
    pieces = with_layout_constraint(pieces, Layout(major_to_minor=(0, 1, 2)))
    mine = lax.dynamic_slice_in_dim(analysis_weights[0], me_mem * mem_dev, mem_dev, 1)
    mine = jnp.roll(mine, -me_mem * mem_dev, axis=0)
    mixed = jnp.einsum("klc,km->mlc", pieces, mine, preferred_element_type=f32)
    analysis_members = (mixed + background_mean.astype(f32)[None]).astype(bf16)

    prior = prior.reshape(mem_dev, channels, obs)
    return (analysis_members, prior.transpose(1, 0, 2))


def solution(mesh):
    fine = Mesh(mesh.devices.reshape(NZ, NX, NC, mesh.devices.shape[1]), TILE + ("mem",))
    placed = (
        P("mem", None, TILE),
        P(TILE, None, None),
        P(None, TILE),
        P("mem", None, TILE),
        P(),
        P(),
        P(TILE, None, None),
        P(TILE, None),
        P(TILE, None),
        P(),
    )
    return jax.shard_map(
        shards,
        mesh=fine,
        in_specs=placed,
        out_specs=(P("mem", None, TILE), P(None, "mem", TILE)),
        check_vma=False,
    )
```

```python
import functools

import jax
import jax.numpy as jnp
from jax import lax
from jax.experimental import pallas as pl
from jax.experimental.layout import Layout, with_layout_constraint
from jax.experimental.pallas import tpu as pltpu
from jax.sharding import Mesh
from jax.sharding import PartitionSpec as P

SLOTS = 32
FOOT = 4
NZ, NX, NC = 8, 4, 2
f32 = jnp.float32
bf16 = jnp.bfloat16
TILE = ("z", "x", "c")
GROUPS = 4
PARTS = (((0,), (1,), (7,)), ((2, 6, 3, 5), (4,)))


def vmem(n):
    return [pl.BlockSpec(memory_space=pltpu.VMEM)] * n


def params(mib=24):
    return pltpu.CompilerParams(vmem_limit_bytes=mib * 2**20)


def radiance_kernel(sel_ref, back_ref, slots_ref, out_ref):
    members, channels = back_ref.shape[0], sel_ref.shape[0]
    sel = sel_ref[...]
    for k in range(members):
        got = jnp.dot(sel, back_ref[k], preferred_element_type=f32)
        out_ref[k * channels : (k + 1) * channels, :] = got.astype(bf16)
    out_ref[members * channels :, :] = slots_ref[...]


def radiance(sel, back, slots):
    rows = back.shape[0] * sel.shape[0] + slots.shape[0]
    return pl.pallas_call(
        radiance_kernel,
        out_shape=pltpu.VMEM((rows, back.shape[2]), bf16),
        in_specs=vmem(3),
        out_specs=vmem(1)[0],
        compiler_params=params(8),
        cost_estimate=pl.CostEstimate(flops=2_000_000_000, bytes_accessed=800_000, transcendentals=0),
        name="radiance",
    )(sel, back, slots)


def pack_kernel(feats, pieces, me_ref, *refs):
    *blocks, out_ref, held, sems = refs
    cols = blocks[0].shape[1]
    peers = out_ref.shape[0]
    tail = blocks[0].shape[0] - feats
    fine = feats // GROUPS
    group = lax.broadcasted_iota(jnp.int32, (8, cols), 1) // SLOTS
    row = lax.broadcasted_iota(jnp.int32, (tail, cols), 0)
    halves = peers // GROUPS
    col = lax.broadcasted_iota(jnp.int32, (cols, cols), 0).astype(f32)
    lane_group = lax.broadcasted_iota(jnp.int32, (cols, cols), 1) // SLOTS
    first, base, stacks = 0, 0, []
    for n in pieces:
        mine = blocks[first : first + n]
        first += n
        rolled = []
        for b in range(GROUPS):
            lists = mine[b % n][feats:, :].astype(f32)
            for h in range(halves):
                line = jnp.sum(jnp.where(row == me_ref[0] * halves + h, lists, 0.0), axis=0, keepdims=True)
                line = jnp.broadcast_to(line, (8, cols))
                rolled.append(pltpu.roll(line, SLOTS * b, 1) if b else line)
        if n == GROUPS:
            left = jnp.concatenate([block[:feats, :] for block in mine], axis=1)
        else:
            left = jnp.concatenate([mine[0][b * fine : (b + 1) * fine, :] for b in range(GROUPS)], axis=1)
        stacks.append((n, left, rolled, base))
        base += feats if n == GROUPS else fine
    copies = []
    for j0 in range(0, peers, 2):
        for n, left, rolled, base in stacks:
            right = []
            for j in (j0, j0 + 1):
                want = jnp.full((8, cols), -1.0, f32)
                for b in range(GROUPS):
                    want = jnp.where(group == (j + b) % GROUPS, rolled[b * halves + j // GROUPS], want)
                same = jnp.broadcast_to(want[0:1, :], (cols, cols)) == col
                turn = j if n == GROUPS else 0
                right.append(
                    jnp.concatenate(
                        [
                            jnp.where(same & (lane_group == (turn + b) % GROUPS), 1.0, 0.0).astype(bf16)
                            for b in range(GROUPS)
                        ],
                        axis=0,
                    )
                )
            got = jnp.dot(left, jnp.concatenate(right, axis=1), preferred_element_type=f32).astype(bf16)
            held[j0, base : base + left.shape[0], :] = got[:, :cols]
            held[j0 + 1, base : base + left.shape[0], :] = got[:, cols:]
        copies.append(pltpu.make_async_copy(held.at[pl.ds(j0, 2)], out_ref.at[pl.ds(j0, 2)], sems.at[j0 // 2]))
        copies[-1].start()
    for copy in copies:
        copy.wait()


def pack(blocks, pieces, me, feats):
    peers, cols = NX * NC, blocks[0].shape[1]
    rows = sum(feats if n == GROUPS else feats // GROUPS for n in pieces)
    return pl.pallas_call(
        functools.partial(pack_kernel, feats, pieces),
        out_shape=pltpu.HBM((peers, rows, cols), bf16),
        in_specs=[pl.BlockSpec(memory_space=pltpu.SMEM)] + vmem(len(blocks)),
        out_specs=pl.BlockSpec(memory_space=pl.ANY),
        scratch_shapes=[pltpu.VMEM((peers, rows, cols), bf16), pltpu.SemaphoreType.DMA((peers // 2,))],
        compiler_params=params(),
        cost_estimate=pl.CostEstimate(flops=2_500_000_000, bytes_accessed=3_000_000, transcendentals=0),
        name="pack",
    )(me, *blocks)


def spread_kernel(row_ref, weight_ref, out_ref):
    rows, obs = out_ref.shape
    step = 128

    @pl.loop(0, rows // step)
    def _(i):
        base = i * step
        row = lax.broadcasted_iota(jnp.int32, (step, obs), 0) + base
        total = jnp.zeros((step, obs), f32)
        for j in range(FOOT):
            total = jnp.where(row == row_ref[j : j + 1, :], weight_ref[j : j + 1, :], total)
        out_ref[pl.ds(pl.multiple_of(base, step), step), :] = total.astype(bf16)


def spread(row, weight, rows):
    return pl.pallas_call(
        spread_kernel,
        out_shape=pltpu.HBM((rows, row.shape[1]), bf16),
        in_specs=vmem(2),
        out_specs=vmem(1)[0],
        compiler_params=params(8),
        cost_estimate=pl.CostEstimate(flops=rows * 1_500_000, bytes_accessed=rows * 1024, transcendentals=0),
        name="spread",
    )(row, weight)


def combine_kernel(count, full, weight_ref, base_ref, got_refs, out_ref):
    step = pl.program_id(0)
    fine, _ = out_ref.shape
    peers, _, width = got_refs[-1].shape
    group = lax.broadcasted_iota(jnp.int32, (fine, width), 1) // SLOTS
    tiles = [got_refs[1][j] for j in range(peers)] if full else []
    for u in range(count):
        for t in range(peers // GROUPS):
            tile = jnp.zeros((fine, width), f32)
            for p in range(GROUPS):
                piece = got_refs[0][t * GROUPS + p, u * fine : (u + 1) * fine, :].astype(f32)
                piece = pltpu.roll(piece, lax.rem(SLOTS * (p - step) + width, width), 1)
                tile = jnp.where(group == p, piece, tile)
            tiles.append(tile.astype(bf16))
    left = jnp.concatenate(tiles, axis=1)
    out_ref[...] = jnp.dot(left, weight_ref[...], preferred_element_type=f32) + base_ref[...]


def combine(got, full, weight, base, mib):
    peers, rows, width = got.shape
    feats, obs = base.shape[0], weight.shape[1]
    fine = feats // GROUPS
    count = rows // fine - (GROUPS if full else 0)
    specs = [pl.BlockSpec((peers, count * fine, width), lambda i: (0, GROUPS if full else 0, 0))]
    if full:
        specs.append(pl.BlockSpec((peers, fine, width), lambda i: (0, i, 0)))

    def body(weight_ref, base_ref, *refs):
        combine_kernel(count, full, weight_ref, base_ref, refs[:-1], refs[-1])

    return pl.pallas_call(
        body,
        grid=(GROUPS,),
        out_shape=pltpu.HBM((feats, obs), f32),
        in_specs=[
            pl.BlockSpec(weight.shape, lambda i: (0, 0)),
            pl.BlockSpec((fine, base.shape[1]), lambda i: (i, 0)),
        ]
        + specs,
        out_specs=pl.BlockSpec((fine, obs), lambda i: (i, 0)),
        compiler_params=params(mib),
        cost_estimate=pl.CostEstimate(flops=4_000_000_000, bytes_accessed=8_000_000, transcendentals=0),
        name="combine",
    )(weight, base, *[got] * len(specs))


def shift(block, axis, size, ahead):
    return lax.ppermute(block, axis, [((i + ahead) % size, i) for i in range(size)])


def ring(block, axis, size):
    blocks, half = {0: block}, size // 2
    for r in range(1, half):
        blocks[r] = shift(blocks[r - 1], axis, size, 1)
        blocks[size - r] = shift(blocks[(size - r + 1) % size], axis, size, size - 1)
    blocks[half] = shift(blocks[half - 1], axis, size, 1)
    return blocks


def shards(
    anomalies,
    analysis_weights,
    background_mean,
    background,
    jacobian_table,
    channel_list,
    send_slots,
    footprint,
    footprint_weight,
    channel_bias,
):
    mem_dev, _, cols = anomalies.shape
    spectrum = jacobian_table.shape[0]
    channels = channel_list.shape[0]
    tiles = send_slots.shape[1]
    obs = footprint.shape[0]
    n_mem = lax.axis_size("mem")
    feats = mem_dev * channels
    peers = NX * NC
    me_z = lax.axis_index("z")
    me_mem = lax.axis_index("mem")

    pick = (channel_list[:, None] == lax.broadcasted_iota(jnp.int32, (channels, spectrum), 1)).astype(bf16)
    selected = jnp.einsum("cv,vl->cl", pick, jacobian_table, preferred_element_type=f32).astype(bf16)
    slots = send_slots[0].reshape(tiles * SLOTS // cols, cols).astype(bf16)
    owned = radiance(selected, background, slots)

    blocks = {0: owned}
    for ahead in (1, 7, 2, 6):
        blocks[ahead] = shift(owned, "z", NZ, ahead)
    blocks[3] = shift(blocks[2], "z", NZ, 1)
    blocks[5] = shift(blocks[6], "z", NZ, 7)
    blocks[4] = shift(blocks[2], "z", NZ, 2)

    slot = footprint.T
    ahead = (slot // (peers * SLOTS) - me_z) % NZ
    peer, place = (slot // SLOTS) % peers, slot % SLOTS
    mine = lax.axis_index("x") * NC + lax.axis_index("c")
    weight = footprint_weight.T.astype(f32)
    prior = jnp.broadcast_to(channel_bias[None, :, None], (mem_dev, channels, 1)).reshape(feats, 1)
    for part in PARTS:
        sent = pack([blocks[r] for piece in part for r in piece], tuple(map(len, part)), me_z.reshape(1), feats)
        got = lax.all_to_all(sent, ("x", "c"), 0, 0)
        row, at = jnp.full((FOOT, obs), -1, jnp.int32), 0
        for piece in part:
            if len(piece) == GROUPS:
                for b, r in enumerate(piece):
                    row = jnp.where(ahead == r, (peer * GROUPS + (mine + b) % GROUPS) * SLOTS + place, row)
            else:
                row = jnp.where(ahead == piece[0], at + peer * SLOTS + place, row)
            at += peers * SLOTS * len(piece)
        matrix = spread(row, weight, at)
        prior = combine(got, len(part[0]) == GROUPS, matrix, prior, 60)

    pieces = ring(anomalies, "mem", n_mem)
    pieces = jnp.concatenate([pieces[r] for r in range(n_mem)], axis=0)
    pieces = with_layout_constraint(pieces, Layout(major_to_minor=(0, 1, 2)))
    mine = lax.dynamic_slice_in_dim(analysis_weights[0], me_mem * mem_dev, mem_dev, 1)
    mine = jnp.roll(mine, -me_mem * mem_dev, axis=0)
    mixed = jnp.einsum("klc,km->mlc", pieces, mine, preferred_element_type=f32)
    analysis_members = (mixed + background_mean.astype(f32)[None]).astype(bf16)

    prior = prior.reshape(mem_dev, channels, obs)
    return (analysis_members, prior.transpose(1, 0, 2))


def solution(mesh):
    fine = Mesh(mesh.devices.reshape(NZ, NX, NC, mesh.devices.shape[1]), TILE + ("mem",))
    placed = (
        P("mem", None, TILE),
        P(TILE, None, None),
        P(None, TILE),
        P("mem", None, TILE),
        P(),
        P(),
        P(TILE, None, None),
        P(TILE, None),
        P(TILE, None),
        P(),
    )

    return jax.shard_map(
        shards,
        mesh=fine,
        in_specs=placed,
        out_specs=(P("mem", None, TILE), P(None, "mem", TILE)),
        check_vma=False,
    )
```

```python
import functools

import jax
import jax.numpy as jnp
from jax import lax
from jax.experimental import pallas as pl
from jax.experimental.layout import Layout, with_layout_constraint
from jax.experimental.pallas import tpu as pltpu
from jax.sharding import Mesh
from jax.sharding import PartitionSpec as P

SLOTS = 32
FOOT = 4
NZ, NX, NC = 8, 4, 2
f32 = jnp.float32
bf16 = jnp.bfloat16
TILE = ("z", "x", "c")
GROUPS = 4
PARTS = (((0,), (1,), (7,)), ((2, 6, 3, 5), (4,)))


def vmem(n):
    return [pl.BlockSpec(memory_space=pltpu.VMEM)] * n


def params(mib=24):
    return pltpu.CompilerParams(vmem_limit_bytes=mib * 2**20)


def radiance_kernel(sel_ref, back_ref, slots_ref, out_ref):
    members, channels = back_ref.shape[0], sel_ref.shape[0]
    sel = sel_ref[...]
    for k in range(members):
        got = jnp.dot(sel, back_ref[k], preferred_element_type=f32)
        out_ref[k * channels : (k + 1) * channels, :] = got.astype(bf16)
    out_ref[members * channels :, :] = slots_ref[...]


def radiance(sel, back, slots):
    rows = back.shape[0] * sel.shape[0] + slots.shape[0]
    return pl.pallas_call(
        radiance_kernel,
        out_shape=jax.ShapeDtypeStruct((rows, back.shape[2]), bf16),
        in_specs=vmem(3),
        out_specs=vmem(1)[0],
        compiler_params=params(6),
        cost_estimate=pl.CostEstimate(flops=2_000_000_000, bytes_accessed=800_000, transcendentals=0),
        name="radiance",
    )(sel, back, slots)


def pack_kernel(feats, pieces, at, me_ref, *refs):
    *blocks, out_ref, held, sems = refs
    blocks = blocks[: sum(pieces)]
    cols = blocks[0].shape[1]
    peers = out_ref.shape[0]
    tail = blocks[0].shape[0] - feats
    fine = feats // GROUPS
    group = lax.broadcasted_iota(jnp.int32, (8, cols), 1) // SLOTS
    row = lax.broadcasted_iota(jnp.int32, (tail, cols), 0)
    halves = peers // GROUPS
    col = lax.broadcasted_iota(jnp.int32, (cols, cols), 0).astype(f32)
    lane_group = lax.broadcasted_iota(jnp.int32, (cols, cols), 1) // SLOTS
    first, base, stacks = 0, 0, []
    for n in pieces:
        mine = blocks[first : first + n]
        first += n
        rolled = []
        for b in range(GROUPS):
            lists = mine[b % n][feats:, :].astype(f32)
            for h in range(halves):
                line = jnp.sum(jnp.where(row == me_ref[0] * halves + h, lists, 0.0), axis=0, keepdims=True)
                line = jnp.broadcast_to(line, (8, cols))
                rolled.append(pltpu.roll(line, SLOTS * b, 1) if b else line)
        if n == GROUPS:
            left = jnp.concatenate([block[:feats, :] for block in mine], axis=1)
        else:
            left = jnp.concatenate([mine[0][b * fine : (b + 1) * fine, :] for b in range(GROUPS)], axis=1)
        stacks.append((n, left, rolled, base))
        base += feats if n == GROUPS else fine
    copies = []
    for j0 in range(0, peers, 2):
        for n, left, rolled, base in stacks:
            right = []
            for j in (j0, j0 + 1):
                want = jnp.full((8, cols), -1.0, f32)
                for b in range(GROUPS):
                    want = jnp.where(group == (j + b) % GROUPS, rolled[b * halves + j // GROUPS], want)
                same = jnp.broadcast_to(want[0:1, :], (cols, cols)) == col
                turn = j if n == GROUPS else 0
                right.append(
                    jnp.concatenate(
                        [
                            jnp.where(same & (lane_group == (turn + b) % GROUPS), 1.0, 0.0).astype(bf16)
                            for b in range(GROUPS)
                        ],
                        axis=0,
                    )
                )
            got = jnp.dot(left, jnp.concatenate(right, axis=1), preferred_element_type=f32).astype(bf16)
            held[j0, base : base + left.shape[0], :] = got[:, :cols]
            held[j0 + 1, base : base + left.shape[0], :] = got[:, cols:]
        target = out_ref.at[pl.ds(j0, 2), pl.ds(at, held.shape[1])]
        copies.append(pltpu.make_async_copy(held.at[pl.ds(j0, 2)], target, sems.at[j0 // 2]))
        copies[-1].start()
    for copy in copies:
        copy.wait()


def pack(blocks, pieces, me, feats, at=0, total=None, into=None):
    peers, cols = NX * NC, blocks[0].shape[1]
    rows = sum(feats if n == GROUPS else feats // GROUPS for n in pieces)
    more = () if into is None else (into,)
    return pl.pallas_call(
        functools.partial(pack_kernel, feats, pieces, at),
        out_shape=pltpu.HBM((peers, total or rows, cols), bf16),
        in_specs=[pl.BlockSpec(memory_space=pltpu.SMEM)]
        + vmem(len(blocks))
        + [pl.BlockSpec(memory_space=pl.ANY)] * len(more),
        out_specs=pl.BlockSpec(memory_space=pl.ANY),
        scratch_shapes=[pltpu.VMEM((peers, rows, cols), bf16), pltpu.SemaphoreType.DMA((peers // 2,))],
        input_output_aliases={1 + len(blocks): 0} if more else {},
        compiler_params=params(12),
        cost_estimate=pl.CostEstimate(flops=2_500_000_000, bytes_accessed=3_000_000, transcendentals=0),
        name="pack",
    )(me, *blocks, *more)


def spread_kernel(row_ref, weight_ref, out_ref):
    rows, obs = out_ref.shape
    step = 128

    @pl.loop(0, rows // step)
    def _(i):
        base = i * step
        row = lax.broadcasted_iota(jnp.int32, (step, obs), 0) + base
        total = jnp.zeros((step, obs), f32)
        for j in range(FOOT):
            total = jnp.where(row == row_ref[j : j + 1, :], weight_ref[j : j + 1, :], total)
        out_ref[pl.ds(pl.multiple_of(base, step), step), :] = total.astype(bf16)


def spread(row, weight, rows):
    return pl.pallas_call(
        spread_kernel,
        out_shape=pltpu.HBM((rows, row.shape[1]), bf16),
        in_specs=vmem(2),
        out_specs=vmem(1)[0],
        compiler_params=params(6),
        cost_estimate=pl.CostEstimate(flops=rows * 1_500_000, bytes_accessed=rows * 1024, transcendentals=0),
        name="spread",
    )(row, weight)


def combine_kernel(count, full, weight_ref, base_ref, got_refs, out_ref):
    step = pl.program_id(0)
    fine, _ = out_ref.shape
    peers, _, width = got_refs[-1].shape
    group = lax.broadcasted_iota(jnp.int32, (fine, width), 1) // SLOTS
    tiles = [got_refs[1][j] for j in range(peers)] if full else []
    for u in range(count):
        for t in range(peers // GROUPS):
            tile = jnp.zeros((fine, width), f32)
            for p in range(GROUPS):
                piece = got_refs[0][t * GROUPS + p, u * fine : (u + 1) * fine, :].astype(f32)
                piece = pltpu.roll(piece, lax.rem(SLOTS * (p - step) + width, width), 1)
                tile = jnp.where(group == p, piece, tile)
            tiles.append(tile.astype(bf16))
    left = jnp.concatenate(tiles, axis=1)
    out_ref[...] = jnp.dot(left, weight_ref[...], preferred_element_type=f32) + base_ref[...]


def combine(got, full, weight, base, mib):
    peers, rows, width = got.shape
    feats, obs = base.shape[0], weight.shape[1]
    fine = feats // GROUPS
    count = rows // fine - (GROUPS if full else 0)
    hold = lambda a: pltpu.with_memory_space_constraint(a, pltpu.HBM) if full else a
    specs = [pl.BlockSpec((peers, count * fine, width), lambda i: (0, GROUPS if full else 0, 0))]
    if full:
        specs.append(pl.BlockSpec((peers, fine, width), lambda i: (0, i, 0)))

    def body(weight_ref, base_ref, *refs):
        combine_kernel(count, full, weight_ref, base_ref, refs[:-1], refs[-1])

    return pl.pallas_call(
        body,
        grid=(GROUPS,),
        out_shape=pltpu.HBM((feats, obs), f32),
        in_specs=[
            pl.BlockSpec(weight.shape, lambda i: (0, 0)),
            pl.BlockSpec((fine, base.shape[1]), lambda i: (i, 0)),
        ]
        + specs,
        out_specs=pl.BlockSpec((fine, obs), lambda i: (i, 0)),
        compiler_params=params(mib),
        cost_estimate=pl.CostEstimate(flops=4_000_000_000, bytes_accessed=8_000_000, transcendentals=0),
        name="combine",
    )(pltpu.with_memory_space_constraint(weight, pltpu.HBM), hold(base), *[got] * len(specs))


def shift(block, axis, size, ahead):
    return lax.ppermute(block, axis, [((i + ahead) % size, i) for i in range(size)])


def ring(block, axis, size):
    blocks, half = {0: block}, size // 2
    for r in range(1, half):
        blocks[r] = shift(blocks[r - 1], axis, size, 1)
        blocks[size - r] = shift(blocks[(size - r + 1) % size], axis, size, size - 1)
    blocks[half] = shift(blocks[half - 1], axis, size, 1)
    return blocks


def shards(
    anomalies,
    analysis_weights,
    background_mean,
    background,
    jacobian_table,
    channel_list,
    send_slots,
    footprint,
    footprint_weight,
    channel_bias,
):
    mem_dev, _, cols = anomalies.shape
    spectrum = jacobian_table.shape[0]
    channels = channel_list.shape[0]
    tiles = send_slots.shape[1]
    obs = footprint.shape[0]
    n_mem = lax.axis_size("mem")
    feats = mem_dev * channels
    peers = NX * NC
    me_z = lax.axis_index("z")
    me_mem = lax.axis_index("mem")

    pick = (channel_list[:, None] == lax.broadcasted_iota(jnp.int32, (channels, spectrum), 1)).astype(bf16)
    selected = jnp.einsum("cv,vl->cl", pick, jacobian_table, preferred_element_type=f32).astype(bf16)
    slots = send_slots[0].reshape(tiles * SLOTS // cols, cols).astype(bf16)
    owned = radiance(selected, background, slots)

    blocks = {0: owned}
    for ahead in (1, 7, 2, 6):
        blocks[ahead] = shift(owned, "z", NZ, ahead)
    blocks[3] = shift(blocks[2], "z", NZ, 1)
    blocks[5] = shift(blocks[6], "z", NZ, 7)
    blocks[4] = shift(blocks[2], "z", NZ, 2)

    me = me_z.reshape(1)
    fine = feats // GROUPS
    sent = pack([blocks[r] for (r,) in PARTS[0]], (1,) * len(PARTS[0]), me, feats)
    first = lax.all_to_all(sent, ("x", "c"), 0, 0)
    four, (last,) = PARTS[1]
    sent = pack([blocks[r] for r in four], (GROUPS,), me, feats, 0, feats + fine)
    sent = pack([blocks[last]], (1,), me, feats, feats, feats + fine, sent)
    got = [first, lax.all_to_all(sent, ("x", "c"), 0, 0)]

    late = (footprint, footprint_weight, channel_bias, analysis_weights, background_mean)
    mine = lax.axis_index("x") * NC + lax.axis_index("c")
    *late, me_z, mine, me_mem, got[0] = lax.optimization_barrier((*late, me_z, mine, me_mem, got[0]))
    footprint, footprint_weight, channel_bias, analysis_weights, background_mean = late
    slot = footprint.T
    ahead = (slot // (peers * SLOTS) - me_z) % NZ
    peer, place = (slot // SLOTS) % peers, slot % SLOTS
    weight = footprint_weight.T.astype(f32)
    prior = jnp.broadcast_to(channel_bias[None, :, None], (mem_dev, channels, 1)).reshape(feats, 1)
    matrices = []
    for part in PARTS:
        row, at = jnp.full((FOOT, obs), -1, jnp.int32), 0
        for piece in part:
            if len(piece) == GROUPS:
                for b, r in enumerate(piece):
                    row = jnp.where(ahead == r, (peer * GROUPS + (mine + b) % GROUPS) * SLOTS + place, row)
            else:
                row = jnp.where(ahead == piece[0], at + peer * SLOTS + place, row)
            at += peers * SLOTS * len(piece)
        matrices.append(spread(row, weight, at))
    order = (0, 1, 7, 2, 3, 6, 4, 5)
    mixing = lax.dynamic_slice_in_dim(analysis_weights[0], me_mem * mem_dev, mem_dev, 1)
    mixing = jnp.roll(mixing, -me_mem * mem_dev, axis=0)
    mixing = jnp.concatenate([mixing[r * mem_dev : (r + 1) * mem_dev] for r in order], axis=0)
    mean = background_mean.astype(f32)[None]
    *matrices, mixing, mean, anomalies_late = lax.optimization_barrier((*matrices, mixing, mean, anomalies))
    for p, part in enumerate(PARTS):
        prior = combine(got[p], len(part[0]) == GROUPS, matrices[p], prior, 12)

    pieces = ring(anomalies, "mem", n_mem)
    pieces[0] = anomalies_late
    pieces = jnp.concatenate([pieces[r] for r in order], axis=0)
    pieces = with_layout_constraint(pieces, Layout(major_to_minor=(0, 1, 2)))
    mixed = jnp.einsum("klc,km->mlc", pieces, mixing, preferred_element_type=f32)
    analysis_members = (mixed + mean).astype(bf16)

    prior = prior.reshape(mem_dev, channels, obs)
    return (analysis_members, prior.transpose(1, 0, 2))


def solution(mesh):
    fine = Mesh(mesh.devices.reshape(NZ, NX, NC, mesh.devices.shape[1]), TILE + ("mem",))
    placed = (
        P("mem", None, TILE),
        P(TILE, None, None),
        P(None, TILE),
        P("mem", None, TILE),
        P(),
        P(),
        P(TILE, None, None),
        P(TILE, None),
        P(TILE, None),
        P(),
    )

    return jax.shard_map(
        shards,
        mesh=fine,
        in_specs=placed,
        out_specs=(P("mem", None, TILE), P(None, "mem", TILE)),
        check_vma=False,
    )
```
